32 devices in a mesh: src: 4 (over y, x), blk: 8 (over z, core).
Axes of the slice: x: 2, y: 2, z: 4, core: 2. Of those that a mesh axis runs over, the one named last changes fastest.
Arguments:
- values: float32 [4, 512, 32, 128], P('src', 'blk'), may hold values from -0.25 to 0.25
- diagonal: float32 [4, 512, 128], P('src', 'blk'), may hold values from 0.55 to 0.95
- rhs_parts: float32 [4, 512, 128], P('src', 'blk'), may hold values from -24 to 24
- owner_map: int32 [512, 128], P('blk'), may hold values from 0 to 3
- columns: int32 [512, 32, 128], P('blk'), may hold values from 0 to 1073741823
- destination: int32 [512, 1], P('blk'), may hold values from 0 to 7; in each aligned block of 64 rows (0 to 63, 64 to 127, ...) at most 16 rows name the same one
- order_keys: int32 [512], P('blk'), may hold values from 0 to 511, each once
Outputs:
- solution: float32 [512, 128], P('blk')
The draws below stay inside these ranges and needn't reach their ends.
Inputs may be any that keep to these rules, and one draw needn't show every extreme that they name: `destination`: among the row blocks of one index of blk no owner is named more than 16 times, some owner is named exactly 16 times, and every owner is named by some block. `order_keys`: each key appears once.
All inputs are finite; a program needn't handle non-finite values.
Results may differ from the reference program's by a relative error of at most 0.0003.
Values sent between devices are 32-bit elements; how exact they have to be, the bound alone decides.
A program may use at most 64 MiB of HBM per device.

```python
import math
import jax
import jax.numpy as jnp
import numpy as np
from jax import lax

TD = 64
TR = 128
KOFF = 32
SWEEPS = 3
SEND = 16
TILES = 512
N_SRC = 4
N_BLK = 8


def with_ends(array, key, low, top_value):
    index_at = [jax.random.randint(jax.random.fold_in(key, axis), (), 0, length) for axis, length in enumerate(array.shape)]
    widest = array.shape.index(max(array.shape))
    beside = index_at[:widest] + [(index_at[widest] + 1) % array.shape[widest]] + index_at[widest + 1:]
    return array.at[tuple(index_at)].set(low).at[tuple(beside)].set(top_value)


def levels(stream_key, dims, shards, least, high):
    def one(dim, shards_of):
        heights = jax.random.uniform(jax.random.fold_in(jax.random.fold_in(stream_key, 6), dim), (shards_of,), jnp.float32, least / len(shards), high / len(shards))
        return jnp.repeat(jnp.exp(heights), dims[dim] // shards_of).reshape((-1,) + (1,) * (len(dims) - dim - 1))

    gain = one(*shards[0])
    for cut in shards[1:]:
        gain = gain * one(*cut)
    return gain


def routed_block(rng, own, number, rows, number_of, top, most, slope):
    order = jax.random.permutation(rng, number_of)
    crowded, usual = shares(number_of, rows * top, most, slope, True), shares(number_of, rows * top, most, slope, False)
    places = jnp.arange(number_of)

    def named(sizes, rotation):
        used = int((sizes > 0).sum())
        fixed = max(1, used // 4)
        moved = fixed + (places - fixed + rotation * (used - fixed)) % max(1, number_of - fixed)
        return jnp.zeros((number_of,), jnp.int32).at[order[jnp.where(places < fixed, places, moved)]].set(jnp.asarray(sizes, jnp.int32))

    sizes = jnp.where(number % 4 == 0, named(crowded, number // 4), named(usual, number - number // 4 - 1))
    mixed = jax.random.permutation(jax.random.fold_in(own, 3), number_of)
    donor, taker = mixed[0:number_of // 2 * 2:2], mixed[1:number_of // 2 * 2:2]
    room = jnp.minimum(sizes[donor] - 1, most - sizes[taker]) // 2
    room = jnp.where((donor == order[0]) | (taker == order[0]) | (sizes[taker] == 0), 0, jnp.maximum(room, 0))
    moved = jax.random.randint(jax.random.fold_in(own, 4), (number_of // 2,), 0, 1 << 20) % (room + 1)
    sizes = sizes.at[donor].add(-moved).at[taker].add(moved)
    members = jnp.searchsorted(jnp.cumsum(sizes), jnp.arange(rows * top), side="right").astype(jnp.int32)
    listing = members.reshape(top, rows).T
    listing = listing[jax.random.permutation(jax.random.fold_in(own, 1), rows)]
    rotation = jax.random.randint(jax.random.fold_in(own, 2), (rows, 1), 0, top)
    return jnp.take_along_axis(listing, (jnp.arange(top)[None, :] + rotation) % top, axis=1)


def shares(number_of, total, most, slope, full):
    loads = [(1 << 20) // math.isqrt(grade ** slope) + 1 for grade in range(1, number_of + 1)]
    largest = most if full else min(most, max(-(-total // number_of), total * loads[0] // sum(loads)))
    least = 1 if total - largest >= number_of - 1 else 0
    given, spare = [largest] + [least] * (number_of - 1), total - largest - least * (number_of - 1)
    while spare > 0:
        free = [i for i in range(1, number_of) if given[i] < largest] or [i for i in range(1, number_of) if given[i] < most]
        whole, budget = sum([loads[i] for i in free]), spare
        for i in free:
            extra = min(most - given[i], max(1, budget * loads[i] // whole), spare)
            given[i] = given[i] + extra
            spare = spare - extra
    return np.array(given)


def gaussian(rng, dims, scale, limit, shards=(), kind=jnp.bfloat16):
    loudness = levels(rng, dims, shards, -0.22, 0.18) if shards else 1.0
    result = jax.random.normal(rng, dims, jnp.float32) * scale * loudness
    return jnp.minimum(jnp.maximum(result, -limit), limit).astype(kind)


def setup_inputs(seed: int = 0) -> dict:
    splits = jax.random.split(jax.random.key(seed), 8)
    values = jnp.clip(jax.random.uniform(splits[0], (N_SRC, TILES, KOFF, TR), jnp.float32, -0.25, 0.25) * levels(splits[0], (N_SRC, TILES, KOFF, TR), ((0, 4), (1, 8)), -0.4, 0.0), -0.25, 0.25)
    diagonal = jnp.clip(0.55 + 0.39999998 * jax.random.uniform(splits[1], (N_SRC, TILES, TR), jnp.float32) ** levels(splits[1], (N_SRC, TILES, TR), ((0, 4), (1, 8)), -0.2, 0.2), 0.55, 0.95)
    rhs_parts = gaussian(splits[2], (N_SRC, TILES, TR), 4.0, 24.0, ((0, 4), (1, 8)), jnp.float32)
    owner_map = with_ends(jax.random.randint(splits[3], (TILES, TR), 0, N_SRC), jax.random.fold_in(splits[3], 1), 0, N_SRC - 1).astype(jnp.int32)
    columns = with_ends(jax.random.randint(splits[4], (TILES, KOFF, TR), 0, 1073741824), jax.random.fold_in(splits[4], 1), 0, 1073741823).astype(jnp.int32)
    destination_keys = jax.random.split(jax.random.fold_in(splits[5], 1), TILES // TD)
    destination_turns = jax.random.permutation(jax.random.fold_in(splits[5], 3), TILES // TD)
    destination = jax.vmap(lambda own, number: routed_block(jax.random.fold_in(splits[5], 2), own, number, TD, N_BLK, 1, SEND, 2))(destination_keys, destination_turns).reshape((TILES, 1))
    order_keys = jax.random.permutation(splits[6], TILES).astype(jnp.int32)
    return dict(values=values, diagonal=diagonal, rhs_parts=rhs_parts, owner_map=owner_map, columns=columns, destination=destination, order_keys=order_keys)


def reference(values, diagonal, rhs_parts, owner_map, columns, destination, order_keys):
    owner_of = destination[:, 0]
    same_owner = owner_of[:, None] == owner_of[None, :]
    tile_rank = jnp.sum(same_owner & (order_keys[None, :] < order_keys[:, None]), axis=1).astype(jnp.int32)
    owner_ids = jnp.arange(N_BLK, dtype=jnp.int32)
    owner_counts = jnp.sum(owner_of[None, :] == owner_ids[:, None], axis=1).astype(jnp.int32)
    slot_count = N_BLK * SEND
    slot_table = jnp.full((N_BLK, slot_count), -1, jnp.int32)
    slot_table = slot_table.at[owner_of, tile_rank].set(jnp.arange(TILES, dtype=jnp.int32))
    assembled = jnp.sum(values, axis=0)
    assembled_diag = jnp.sum(diagonal, axis=0)
    right_side = jnp.take_along_axis(rhs_parts, owner_map[None, :, :], axis=0)[0]
    slot_numbers = jnp.arange(slot_count, dtype=jnp.int32)

    def solve_owner(owner):
        chosen = slot_table[owner]
        is_live = chosen >= 0
        safe_index = jnp.maximum(chosen, 0)
        block_vals = jnp.where(is_live[:, None, None], assembled[safe_index], 0.0)
        block_cols = columns[safe_index]
        block_right = jnp.where(is_live[:, None], right_side[safe_index], 0.0)
        block_diag = jnp.where(is_live[:, None], assembled_diag[safe_index], 1.0)
        step_over = jnp.remainder(block_cols // TR, 2).astype(jnp.int32)
        target_tile = jnp.remainder(slot_numbers[:, None, None] + step_over, owner_counts[owner]).astype(jnp.int32)
        location = (target_tile * TR + jnp.remainder(block_cols, TR)).astype(jnp.int32)
        iterate = jnp.zeros((slot_count * TR,), jnp.float32)
        for sweep_index in range(SWEEPS):
            nearby = iterate[location]
            summed = jnp.sum(block_vals * nearby, axis=1)
            update = jnp.where(is_live[:, None], (block_right - summed) / block_diag, 0.0)
            iterate = update.reshape(-1)
        return iterate.reshape(slot_count, TR)

    solved = lax.map(solve_owner, owner_ids)
    return solved[owner_of, tile_rank]
```

```python
import functools
import jax
import jax.numpy as jnp
from jax import lax
from jax.experimental import pallas as pl
from jax.experimental.pallas import tpu as pltpu
from jax.sharding import PartitionSpec as P

SWEEPS = 3
PIECES = 2
HALVES = 2


def kernel(n_src, n_blk, values_hbm, columns_hbm, diag_hbm, rhs_hbm, map_hbm, dest_hbm, keys_hbm, out_ref,
           vals, mat_in, cols, dr, map_ref, dest_ref, keys_ref, comb_all, comb_sum,
           iterate, snd, rcv, far, acc, psnd, prcv, total_ref,
           load_sem, comb_send, comb_recv, dr_send, dr_recv, mat_send, mat_recv,
           zed_send, zed_recv, p_send, p_recv):
    s = lax.axis_index("src")
    b = lax.axis_index("blk")
    tiles, rows = map_ref.shape
    stored = vals.shape[1]
    q = tiles // n_src
    lanes = n_blk * q
    total = n_blk * tiles
    piece_q = q // PIECES
    top = n_src // 2
    low_bit = lax.rem(s, 2)
    high_bit = s // top
    near_peer = s + 1 - 2 * low_bit
    side_peer = s + top - 2 * top * high_bit
    both_peer = near_peer + top - 2 * top * high_bit
    src_peers = [near_peer, side_peer, both_peer]
    blk_peers = [lax.rem(b + o, n_blk) for o in range(1, n_blk)]
    mesh_id = pl.DeviceIdType.MESH
    started = []
    mine = [low_bit, top + high_bit]
    other = [1 - low_bit, top + 1 - high_bit]
    partner = [near_peer, side_peer]

    def quarter(part, low=0, size=q):
        return pl.ds(pl.multiple_of(part * q + low, size), size)

    barrier = pltpu.get_barrier_semaphore()
    for peer in src_peers:
        pl.semaphore_signal(barrier, inc=1, device_id={"src": peer}, device_id_type=mesh_id)
    for peer in blk_peers:
        pl.semaphore_signal(barrier, inc=1, device_id={"blk": peer}, device_id_type=mesh_id)
    pairs = [(dest_hbm, dest_ref), (keys_hbm, keys_ref), (diag_hbm, dr.at[s, 0]), (rhs_hbm, dr.at[s, 1]), (map_hbm, map_ref),
             (values_hbm, vals)]
    pairs += [(columns_hbm.at[quarter(mine[h])], cols.at[h]) for h in range(HALVES)]
    loads = [pltpu.make_async_copy(src, dst, load_sem.at[i]) for i, (src, dst) in enumerate(pairs)]
    for load in loads:
        load.start()
    for load in loads[:2]:
        load.wait()

    dest_row = dest_ref[...].astype(jnp.float32)
    comb_row = dest_row * total + keys_ref[...].astype(jnp.float32) + 1.0
    eye = lax.broadcasted_iota(jnp.int32, (tiles, tiles), 0) == lax.broadcasted_iota(jnp.int32, (tiles, tiles), 1)
    comb_col = jnp.sum(jnp.where(eye, comb_row, 0.0), axis=1, keepdims=True)
    low_col = jnp.sum(jnp.where(eye, dest_row, 0.0), axis=1, keepdims=True) * total + 1.0
    at_lane = lax.broadcasted_iota(jnp.int32, (q, lanes), 1) - b * q == lax.broadcasted_iota(jnp.int32, (q, lanes), 0)
    for part in range(n_src):
        spread = jnp.where(at_lane, comb_col[part * q:(part + 1) * q], 0.0)
        comb_all[b, part:part + 1, :] = jnp.sum(spread, axis=0, keepdims=True)
    for load in loads[2:6]:
        load.wait()

    pl.semaphore_wait(barrier, n_src + n_blk - 2)

    def send(src, dst, send_sem, recv_sem, device):
        copy = pltpu.make_async_remote_copy(src_ref=src, dst_ref=dst, send_sem=send_sem, recv_sem=recv_sem,
                                            device_id=device, device_id_type=mesh_id)
        copy.start()
        started.append(copy)

    def arrive(dst, send_sem, recv_sem, device):
        pltpu.make_async_remote_copy(src_ref=dst, dst_ref=dst, send_sem=send_sem, recv_sem=recv_sem,
                                     device_id=device, device_id_type=mesh_id).wait_recv()

    for peer in blk_peers:
        send(comb_all.at[b], comb_all.at[b], comb_send.at[peer], comb_recv.at[b], {"blk": peer})
    for peer in src_peers:
        send(dr.at[s], dr.at[s], dr_send.at[peer], dr_recv.at[s], {"src": peer})
    for piece in range(PIECES):
        for h in range(HALVES):
            there = quarter(other[h], piece * piece_q, piece_q)
            here = pl.ds(piece * piece_q, piece_q)
            send(vals.at[there], mat_in.at[h, here], mat_send.at[h, piece], mat_recv.at[h, piece], {"src": partner[h]})

    for peer in blk_peers:
        arrive(comb_all.at[peer], comb_send.at[peer], comb_recv.at[peer], {"blk": peer})
    all_combs = comb_all[0]
    for one in range(1, n_blk):
        all_combs = all_combs + comb_all[one]
    comb_sum[...] = all_combs
    before = jnp.zeros((tiles, lanes), jnp.float32)
    last = jnp.zeros((tiles, lanes), jnp.float32)
    for part in range(n_src):
        line = comb_sum[part:part + 1, :]
        owned = jnp.where((line >= low_col) & (line < low_col + total), line, 0.0)
        before = jnp.maximum(before, jnp.where(owned < comb_col, owned, 0.0))
        last = jnp.maximum(last, owned)
    before = jnp.max(before, axis=1, keepdims=True)
    last = jnp.max(last, axis=1, keepdims=True)
    previous = jnp.where(before > 0.0, before, last)
    choices = []
    for h in range(HALVES):
        chosen = jnp.where(comb_sum[pl.ds(mine[h], 1), :] == previous, 1.0, 0.0)
        choices.append(jnp.concatenate([chosen] * 3, axis=0).T.astype(jnp.bfloat16))

    def share(step, x):
        iterate[...] = x
        high = x.astype(jnp.bfloat16)
        rest = x - high.astype(jnp.float32)
        middle = rest.astype(jnp.bfloat16)
        small = (rest - middle.astype(jnp.float32)).astype(jnp.bfloat16)
        parts = jnp.concatenate([high, middle, small], axis=0)
        for h in range(HALVES):
            got = jnp.dot(choices[h], parts, preferred_element_type=jnp.float32)
            snd[step, :, h] = got.reshape(n_blk, q, rows)
        for peer in blk_peers:
            send(snd.at[step, peer], rcv.at[step, b], zed_send.at[step, peer], zed_recv.at[step, b], {"blk": peer})

    def product(h, low, size, vector, start, take_far, first):
        def block(i, carry):
            t = low + i
            code = cols[h, t]
            entry = vals[mine[h] * q + t]
            if first:
                entry = entry + mat_in[h, t]
                vals[mine[h] * q + t] = entry
            x = jnp.broadcast_to(vector[pl.ds(start + t, 1), :], (stored, rows))
            got = jnp.take_along_axis(x, code & (rows - 1), axis=1, mode="promise_in_bounds")
            wanted = (code & rows) != 0 if take_far else (code & rows) == 0
            term = jnp.where(wanted, got * entry, 0.0)
            slim = jnp.sum(term.reshape(stored // 8, 8, rows), axis=0)
            acc[h, t] = acc[h, t] + slim if take_far else slim
            return carry

        lax.fori_loop(0, size, block, 0, unroll=8)

    for peer in src_peers:
        arrive(dr.at[peer], dr_send.at[peer], dr_recv.at[peer], {"src": peer})
    diag = dr[0, 0]
    for one in range(1, n_src):
        diag = diag + dr[one, 0]
    owner = map_ref[...]
    right = jnp.where(owner == 0, dr[0, 1], 0.0)
    for one in range(1, n_src):
        right = jnp.where(owner == one, dr[one, 1], right)

    share(0, right / diag)
    for load in loads[6:]:
        load.wait()

    for step in range(SWEEPS - 1):
        for piece in range(PIECES):
            for h in range(HALVES):
                here = pl.ds(piece * piece_q, piece_q)
                if step == 0:
                    arrive(mat_in.at[h, here], mat_send.at[h, piece], mat_recv.at[h, piece], {"src": partner[h]})
                product(h, piece * piece_q, piece_q, iterate, mine[h] * q, False, step == 0)
        for peer in blk_peers:
            arrive(rcv.at[step, peer], zed_send.at[step, peer], zed_recv.at[step, peer], {"blk": peer})
        ahead = snd[step, b]
        for peer in blk_peers:
            ahead = ahead + rcv[step, peer]
        far[...] = ahead.reshape(HALVES * q, rows)
        for h in range(HALVES):
            product(h, 0, q, far, h * q, True, False)
        psnd[step] = jnp.sum(acc[...], axis=2)
        for peer in src_peers:
            send(psnd.at[step], prcv.at[step, s], p_send.at[step, peer], p_recv.at[step, s], {"src": peer})
        for peer in src_peers:
            arrive(prcv.at[step, peer], p_send.at[step, peer], p_recv.at[step, peer], {"src": peer})
        total_ref[quarter(mine[0]), :] = psnd[step, 0] + prcv[step, side_peer, 0]
        total_ref[quarter(mine[1]), :] = psnd[step, 1] + prcv[step, near_peer, 1]
        total_ref[quarter(other[0]), :] = prcv[step, near_peer, 0] + prcv[step, both_peer, 0]
        total_ref[quarter(other[1]), :] = prcv[step, side_peer, 1] + prcv[step, both_peer, 1]
        x = (right - total_ref[...]) / diag
        if step < SWEEPS - 2:
            share(step + 1, x)
    out_ref[...] = x
    for copy in started:
        copy.wait_send()


def on_device(values, diagonal, rhs_parts, owner_map, columns, destination, order_keys):
    n_src = lax.axis_size("src")
    n_blk = lax.axis_size("blk")
    tiles, rows = diagonal.shape[1:]
    stored = values.shape[2]
    q = tiles // n_src
    f32 = jnp.float32
    i32 = jnp.int32
    dma = pltpu.SemaphoreType.DMA
    later = SWEEPS - 1
    return pl.pallas_call(
        functools.partial(kernel, n_src, n_blk),
        out_shape=pltpu.VMEM((tiles, rows), f32),
        in_specs=[pl.BlockSpec(memory_space=pl.ANY)] * 7,
        out_specs=pl.BlockSpec(memory_space=pltpu.VMEM),
        scratch_shapes=[
            pltpu.VMEM((tiles, stored, rows), f32),
            pltpu.VMEM((HALVES, q, stored, rows), f32),
            pltpu.VMEM((HALVES, q, stored, rows), i32),
            pltpu.VMEM((n_src, 2, tiles, rows), f32),
            pltpu.VMEM((tiles, rows), i32),
            pltpu.VMEM((1, tiles), i32),
            pltpu.VMEM((1, tiles), i32),
            pltpu.VMEM((n_blk, n_src, n_blk * q), f32),
            pltpu.VMEM((n_src, n_blk * q), f32),
            pltpu.VMEM((tiles, rows), f32),
            pltpu.VMEM((later, n_blk, HALVES, q, rows), f32),
            pltpu.VMEM((later, n_blk, HALVES, q, rows), f32),
            pltpu.VMEM((HALVES * q, rows), f32),
            pltpu.VMEM((HALVES, q, 8, rows), f32),
            pltpu.VMEM((later, HALVES, q, rows), f32),
            pltpu.VMEM((later, n_src, HALVES, q, rows), f32),
            pltpu.VMEM((tiles, rows), f32),
            dma((8,)),
            dma((n_blk,)), dma((n_blk,)),
            dma((n_src,)), dma((n_src,)),
            dma((HALVES, PIECES)), dma((HALVES, PIECES)),
            dma((later, n_blk)), dma((later, n_blk)),
            dma((later, n_src)), dma((later, n_src)),
        ],
        compiler_params=pltpu.CompilerParams(collective_id=0, has_side_effects=True),
    )(values[0], columns, diagonal[0], rhs_parts[0], owner_map, destination.reshape(1, tiles), order_keys.reshape(1, tiles))


def solution(mesh):
    placed = (
        P("src", "blk", None, None),
        P("src", "blk", None),
        P("src", "blk", None),
        P("blk", None),
        P("blk", None, None),
        P("blk", None),
        P("blk"),
    )
    return jax.shard_map(
        on_device, mesh=mesh, in_specs=placed, out_specs=P("blk", None), check_vma=False
    )
```
